32 devices in a mesh: row: 4 (over x, core), col: 4 (over z), head: 2 (over y).
Axes of the slice: x: 2, y: 2, z: 4, core: 2. Of those that a mesh axis runs over, the one named last changes fastest.
Arguments:
- query_map: bfloat16 [64, 128, 3072], P('row', 'col', 'head'), may hold values from -6 to 6
- key_map: bfloat16 [64, 128, 3072], P('row', 'col', 'head'), may hold values from -7 to 7
- value_map: bfloat16 [64, 128, 3072], P('row', 'col', 'head'), may hold values from -6 to 6
- window_mask: int32 [4, 4, 13, 13], P('row', 'col'), may hold values 0 or 1
- tile_radius: int32 [4, 4], P('row', 'col'), may hold values from 3 to 6, as said below
- dilation_per_tile: int32 [4, 4], P('row', 'col'), may hold values from 1 to 3, as said below
- rel_bias: float32 [48, 13, 13], P('head'), may hold values from -4 to 4
- out_weight: bfloat16 [3072, 3072], P('head'), may hold values from -0.109375 to 0.109375
Outputs:
- mixed: bfloat16 [64, 128, 3072], P('row', 'col', 'head')
The draws below stay inside these ranges and needn't reach their ends.
Inputs may be any that keep to these rules, and one draw needn't show every extreme that they name: `tile_radius`: in each row of tiles, at least one tile has radius 6 and dilation 3. `dilation_per_tile`: in each row of tiles, at least one tile has radius 6 and dilation 3.
All inputs are finite; a program needn't handle non-finite values. No bound on the sum of `window_mask` on one device may be relied on, other than what follows from the above.
Results may differ from the reference program's by a relative error of at most 0.0073.
Values may be sent and summed in bfloat16 or wider, within the bound.
A program may use at most 384 MiB of HBM per device.

```python
import math
from functools import partial
import jax
import jax.numpy as jnp
from jax import lax

TILE_ROWS = 16
TILE_COLS = 32
HEADS = 48
HEAD_DIM = 64
RADIUS_MAX = 6
DILATION_LIMIT = 3
WINDOW = 13
HALO = 18
FEATURES = 3072
MODEL = 3072
ROWS = 64
COLS = 128
N_ROW = 4
N_COL = 4


def draw_query_map(key, part):
    drawn = jax.random.normal(jax.random.fold_in(key, 3), (ROWS, COLS, FEATURES), jnp.float32)
    return jnp.clip(drawn, -6.0, 6.0).astype(jnp.bfloat16)


def draw_key_map(key, part):
    drawn = jax.random.normal(jax.random.fold_in(key, 5), (ROWS, COLS, FEATURES), jnp.float32)
    return jnp.clip(drawn, -6.0, 6.0).astype(jnp.bfloat16)


def window_settings(key):
    base = jax.random.fold_in(key, 29)
    pick_key, radius_key, dilation_key = jax.random.split(base, 3)
    chosen_col = jax.random.randint(pick_key, (N_ROW,), 0, N_COL)
    radius = jax.random.randint(radius_key, (N_ROW, N_COL), 3, RADIUS_MAX + 1)
    dilation = jax.random.randint(dilation_key, (N_ROW, N_COL), 1, DILATION_LIMIT + 1)
    widest = jnp.arange(N_COL, dtype=jnp.int32)[None, :] == chosen_col[:, None]
    radius = jnp.where(widest, RADIUS_MAX, radius).astype(jnp.int32)
    dilation = jnp.where(widest, DILATION_LIMIT, dilation).astype(jnp.int32)
    return (radius, dilation)


def draw_tile_radius(key, part):
    return window_settings(key)[0]


def draw_dilation_per_tile(key, part):
    return window_settings(key)[1]


def touch_ends(result, own_key, smallest, top_value):
    index_at = [jax.random.randint(jax.random.fold_in(own_key, axis), (), 0, length) for axis, length in enumerate(result.shape)]
    longest = result.shape.index(max(result.shape))
    next_to = index_at[:longest] + [(index_at[longest] + 1) % result.shape[longest]] + index_at[longest + 1:]
    return result.at[tuple(index_at)].set(smallest).at[tuple(next_to)].set(top_value)


def shard_levels(key, shape, cuts, low, high):
    gain, own = 1.0, jax.random.fold_in(key, 6)
    for position, parts in cuts:
        draws = jnp.exp(jax.random.uniform(jax.random.fold_in(own, position), (parts,), jnp.float32, low / len(cuts), high / len(cuts)))
        gain = gain * jnp.repeat(draws, shape[position] // parts).reshape([-1 if axis == position else 1 for axis in range(len(shape))])
    return gain


def gaussian(rng, dims, width, limit, pieces=(), kind=jnp.bfloat16):
    values = width * jax.random.normal(rng, dims, jnp.float32)
    if pieces:
        values = values * shard_levels(rng, dims, pieces, -0.22, 0.18)
    return jnp.clip(values, -limit, limit).astype(kind)


def setup_inputs(seed: int = 0) -> dict:
    keys = jax.random.split(jax.random.key(seed), 9)
    query_map = draw_query_map(jax.random.fold_in(keys[8], 71), 0)
    key_map = draw_key_map(jax.random.fold_in(keys[8], 71), 0)
    value_map = gaussian(keys[2], (ROWS, COLS, FEATURES), 1.0, 6.0, ((0, 4), (1, 4), (2, 2)))
    window_mask = touch_ends((jax.random.randint(keys[3], (N_ROW, N_COL, WINDOW, WINDOW), 0, 4) < 3).astype(jnp.int32), jax.random.fold_in(keys[3], 1), 0, 1)
    tile_radius = draw_tile_radius(jax.random.fold_in(keys[8], 71), 0)
    dilation_per_tile = draw_dilation_per_tile(jax.random.fold_in(keys[8], 71), 0)
    rel_bias = gaussian(keys[6], (HEADS, WINDOW, WINDOW), 1.0, 4.0, ((0, 2),), jnp.float32)
    out_weight = gaussian(keys[7], (FEATURES, MODEL), FEATURES ** -0.5, 0.109375, ((0, 2),))
    return {"query_map": query_map, "key_map": key_map, "value_map": value_map, "window_mask": window_mask, "tile_radius": tile_radius, "dilation_per_tile": dilation_per_tile, "rel_bias": rel_bias, "out_weight": out_weight}


def tile_attention(index, query_map, padded_keys, padded_values, window_mask, tile_radius, dilation_per_tile, rel_bias):
    tile_row = index // N_COL
    tile_col = index % N_COL
    row_anchor = tile_row * TILE_ROWS
    col_anchor = tile_col * TILE_COLS
    zero_index = jnp.int32(0)
    queries = lax.dynamic_slice(query_map, (row_anchor, col_anchor, zero_index), (TILE_ROWS, TILE_COLS, FEATURES))
    queries = queries.astype(jnp.float32).reshape(TILE_ROWS, TILE_COLS, HEADS, HEAD_DIM)
    key_block = lax.dynamic_slice(padded_keys, (row_anchor, col_anchor, zero_index), (TILE_ROWS + 2 * HALO, TILE_COLS + 2 * HALO, FEATURES))
    value_block = lax.dynamic_slice(padded_values, (row_anchor, col_anchor, zero_index), (TILE_ROWS + 2 * HALO, TILE_COLS + 2 * HALO, FEATURES))
    radius = tile_radius[tile_row, tile_col]
    dilation = dilation_per_tile[tile_row, tile_col]
    pattern = window_mask[tile_row, tile_col]
    rows_here = row_anchor + jnp.arange(TILE_ROWS, dtype=jnp.int32)
    cols_here = col_anchor + jnp.arange(TILE_COLS, dtype=jnp.int32)
    score_scale = 1.0 / math.sqrt(HEAD_DIM)
    score_list = []
    mask_list = []
    starts = []
    for row_step in range(-RADIUS_MAX, RADIUS_MAX + 1):
        for col_step in range(-RADIUS_MAX, RADIUS_MAX + 1):
            row_start = HALO + row_step * dilation
            col_start = HALO + col_step * dilation
            starts.append((row_start, col_start))
            shifted = lax.dynamic_slice(key_block, (row_start, col_start, zero_index), (TILE_ROWS, TILE_COLS, FEATURES))
            shifted = shifted.astype(jnp.float32).reshape(TILE_ROWS, TILE_COLS, HEADS, HEAD_DIM)
            score = lax.optimization_barrier(jnp.sum(queries * shifted, axis=-1)) * score_scale
            score = score + rel_bias[:, row_step + RADIUS_MAX, col_step + RADIUS_MAX][None, None, :]
            inside = pattern[row_step + RADIUS_MAX, col_step + RADIUS_MAX] == 1
            if row_step == 0 and col_step == 0:
                inside = jnp.logical_or(inside, True)
            inside = inside & (abs(row_step) <= radius) & (abs(col_step) <= radius)
            row_global = rows_here + row_step * dilation
            col_global = cols_here + col_step * dilation
            row_fine = (row_global >= 0) & (row_global < ROWS)
            column_offset = (col_global >= 0) & (col_global < COLS)
            mask_list.append(inside & row_fine[:, None] & column_offset[None, :])
            score_list.append(score)
    scores = jnp.stack(score_list)
    masks = jnp.stack(mask_list)[..., None]
    peak_score = lax.optimization_barrier(jnp.max(jnp.where(masks, scores, -1e+30), axis=0, keepdims=True))
    exponent = jnp.where(masks, jnp.exp(jnp.where(masks, scores - peak_score, -60.0)), 0.0)
    denominator = lax.optimization_barrier(jnp.sum(exponent, axis=0, keepdims=True))
    weights = (exponent / denominator).astype(jnp.bfloat16)
    attended = jnp.zeros((TILE_ROWS, TILE_COLS, HEADS, HEAD_DIM), jnp.float32)
    for place in range(len(starts)):
        row_start, col_start = starts[place]
        shifted = lax.dynamic_slice(value_block, (row_start, col_start, zero_index), (TILE_ROWS, TILE_COLS, FEATURES))
        shifted = shifted.astype(jnp.float32).reshape(TILE_ROWS, TILE_COLS, HEADS, HEAD_DIM)
        attended = attended + weights[place].astype(jnp.float32)[..., None] * shifted
    return attended.reshape(TILE_ROWS, TILE_COLS, FEATURES).astype(jnp.bfloat16)

def reference(query_map, key_map, value_map, window_mask, tile_radius, dilation_per_tile, rel_bias, out_weight):
    padding = ((HALO, HALO), (HALO, HALO), (0, 0))
    padded_keys = jnp.pad(key_map, padding)
    padded_values = jnp.pad(value_map, padding)
    worker = partial(tile_attention, query_map=query_map, padded_keys=padded_keys, padded_values=padded_values, window_mask=window_mask, tile_radius=tile_radius, dilation_per_tile=dilation_per_tile, rel_bias=rel_bias)
    tiles = lax.map(worker, jnp.arange(N_ROW * N_COL, dtype=jnp.int32))
    tiles = tiles.reshape(N_ROW, N_COL, TILE_ROWS, TILE_COLS, FEATURES).transpose(0, 2, 1, 3, 4)
    attended = tiles.reshape(ROWS * COLS, FEATURES)
    mixed = jnp.dot(attended, out_weight, preferred_element_type=jnp.float32).astype(jnp.bfloat16)
    return mixed.reshape(ROWS, COLS, MODEL)
```

```python
import functools
import math

import jax
import jax.numpy as jnp
from jax import lax
from jax.experimental import pallas as pl
from jax.experimental.pallas import tpu as pltpu
from jax.sharding import PartitionSpec as P

HEAD_DIM = 64
RADIUS_MAX = 6
DILATION_LIMIT = 3
WINDOW = 2 * RADIUS_MAX + 1
HALO = RADIUS_MAX * DILATION_LIMIT
GROUP = 4
GROUP_FEATURES = GROUP * HEAD_DIM
MASKED = -1e30

QUERY_COLS = 4
SLOTS = QUERY_COLS + WINDOW - 1
PAIRS = SLOTS // 2
BIAS_STEPS = SLOTS + QUERY_COLS - 2
TABLE_STEPS = BIAS_STEPS + 1
ENTRY = QUERY_COLS + SLOTS + PAIRS

TO_LEFT, TO_RIGHT, TO_ABOVE, TO_BELOW, TOP_UP, BOTTOM_DOWN = range(6)
MATE_LEFT, MATE_RIGHT, ACROSS_LEFT, ACROSS_RIGHT = range(6, 10)
UP_LEFT, UP_RIGHT, DOWN_LEFT, DOWN_RIGHT = range(10, 14)
COPIES = 14


def block_count(cols):
    return max(
        d * -(-(-(-cols // d)) // QUERY_COLS) for d in range(1, DILATION_LIMIT + 1)
    )


def fused_kernel(
    groups, rows, cols, table_ref, slot_ref, bias_ref, step_ref, spread_ref, query_ref,
    kv_hbm, edge_hbm, out_ref, *scratch
):
    kv_refs, edge_refs = scratch[:groups], scratch[groups : 2 * groups]
    tile_ref, done_ref, send_sems, recv_sems, own_sems = scratch[2 * groups :]
    spill = HALO - rows
    own = slice(HALO, HALO + cols)
    left, right = slice(0, HALO), slice(HALO + cols, cols + 2 * HALO)
    row, col = lax.axis_index("row"), lax.axis_index("col")
    n_row, n_col = lax.axis_size("row"), lax.axis_size("col")
    lower = lax.rem(row, 2)
    mate = row + 1 - 2 * lower
    has_left, has_right = col > 0, col < n_col - 1
    has_above, has_below = row > 0, row < n_row - 1
    has_above2, has_below2 = row > 1, row < n_row - 2
    has_mate = mate < n_row
    has_across = jnp.where(lower == 1, has_below, has_above)
    mate_rows = pl.ds(pl.multiple_of((1 + lower) * rows, rows), rows)
    across_rows = pl.ds(pl.multiple_of((1 + lower) * rows, rows), rows)
    edge = spill * cols
    side = -(-spill * HALO // 16) * 16

    def copy(g, which):
        kv, extra = kv_refs[g], edge_refs[g]
        base = slice(0, rows)
        up, down = slice(rows, 2 * rows), slice(2 * rows, 3 * rows)
        near_left, near_right = slice(HALO, 2 * HALO), slice(cols, cols + HALO)
        source, target, there = {
            TO_LEFT: (kv_hbm.at[g, :, :HALO], kv.at[:, right, base], {"col": col - 1}),
            TO_RIGHT: (kv_hbm.at[g, :, cols - HALO :], kv.at[:, left, base], {"col": col + 1}),
            TO_ABOVE: (kv_hbm.at[g], kv.at[:, own, down], {"row": row - 1}),
            TO_BELOW: (kv_hbm.at[g], kv.at[:, own, up], {"row": row + 1}),
            TOP_UP: (edge_hbm.at[g, :, 0], extra.at[:, 1, :edge], {"row": row - 2}),
            BOTTOM_DOWN: (edge_hbm.at[g, :, 1], extra.at[:, 0, :edge], {"row": row + 2}),
            MATE_LEFT: (kv.at[:, left, base], kv.at[:, left, mate_rows], {"row": mate}),
            MATE_RIGHT: (kv.at[:, right, base], kv.at[:, right, mate_rows], {"row": mate}),
            ACROSS_LEFT: (
                kv.at[:, near_left, across_rows], kv.at[:, right, across_rows], {"col": col - 1}
            ),
            ACROSS_RIGHT: (
                kv.at[:, near_right, across_rows], kv.at[:, left, across_rows], {"col": col + 1}
            ),
            UP_LEFT: (
                extra.at[:, 0, :side], extra.at[:, 0, edge + side : edge + 2 * side], {"col": col - 1}
            ),
            UP_RIGHT: (
                extra.at[:, 0, edge - side : edge], extra.at[:, 0, edge : edge + side], {"col": col + 1}
            ),
            DOWN_LEFT: (
                extra.at[:, 1, :side], extra.at[:, 1, edge + side : edge + 2 * side], {"col": col - 1}
            ),
            DOWN_RIGHT: (
                extra.at[:, 1, edge - side : edge], extra.at[:, 1, edge : edge + side], {"col": col + 1}
            ),
        }[which]
        return pltpu.make_async_remote_copy(
            src_ref=source, dst_ref=target, send_sem=send_sems.at[g, which],
            recv_sem=recv_sems.at[g, which], device_id=there,
            device_id_type=pl.DeviceIdType.MESH,
        )

    sends = {
        TO_LEFT: has_left, TO_RIGHT: has_right, TO_ABOVE: has_above, TO_BELOW: has_below,
        TOP_UP: has_above2, BOTTOM_DOWN: has_below2,
        MATE_LEFT: has_mate & has_left, MATE_RIGHT: has_mate & has_right,
        ACROSS_LEFT: has_across & has_left, ACROSS_RIGHT: has_across & has_right,
        UP_LEFT: has_above2 & has_left, UP_RIGHT: has_above2 & has_right,
        DOWN_LEFT: has_below2 & has_left, DOWN_RIGHT: has_below2 & has_right,
    }
    receives = {
        TO_LEFT: has_right, TO_RIGHT: has_left, TO_ABOVE: has_below, TO_BELOW: has_above,
        TOP_UP: has_below2, BOTTOM_DOWN: has_above2,
        MATE_LEFT: has_mate & has_left, MATE_RIGHT: has_mate & has_right,
        ACROSS_LEFT: has_across & has_right, ACROSS_RIGHT: has_across & has_left,
        UP_LEFT: has_above2 & has_right, UP_RIGHT: has_above2 & has_left,
        DOWN_LEFT: has_below2 & has_right, DOWN_RIGHT: has_below2 & has_left,
    }
    first, second = tuple(range(6)), tuple(range(6, COPIES))

    def start(g, kinds):
        for which in kinds:
            @pl.when(sends[which])
            def _():
                copy(g, which).start()

    def arrive(g, kinds):
        for which in kinds:
            @pl.when(receives[which])
            def _():
                copy(g, which).wait_recv()

    def own_copy(g):
        return pltpu.make_async_copy(
            kv_hbm.at[g], kv_refs[g].at[:, own, slice(0, rows)], own_sems.at[g]
        )

    neighbours = (
        (has_left, {"col": col - 1}), (has_right, {"col": col + 1}),
        (has_above, {"row": row - 1}), (has_below, {"row": row + 1}),
        (has_above2, {"row": row - 2}), (has_below2, {"row": row + 2}),
    )
    barrier = pltpu.get_barrier_semaphore()
    for exists, there in neighbours:
        @pl.when(exists)
        def _():
            pl.semaphore_signal(
                barrier, inc=1, device_id=there, device_id_type=pl.DeviceIdType.MESH
            )
    for g in range(groups):
        own_copy(g).start()

    def clear(part):
        part[...] = jnp.zeros(part.shape, part.dtype)

    for g in range(groups):
        kv, extra = kv_refs[g], edge_refs[g]
        for which in range(2):
            @pl.when(jnp.logical_not(has_left))
            def _():
                clear(kv.at[which, left, : 3 * rows])
                for near in range(2):
                    clear(extra.at[which, near, edge : edge + side])

            @pl.when(jnp.logical_not(has_right))
            def _():
                clear(kv.at[which, right, : 3 * rows])
                for near in range(2):
                    clear(extra.at[which, near, edge + side :])

            @pl.when(jnp.logical_not(has_above))
            def _():
                clear(kv.at[which, :, rows : 2 * rows])

            @pl.when(jnp.logical_not(has_below))
            def _():
                clear(kv.at[which, :, 2 * rows : 3 * rows])

            @pl.when(jnp.logical_not(has_above2))
            def _():
                clear(extra.at[which, 0])

            @pl.when(jnp.logical_not(has_below2))
            def _():
                clear(extra.at[which, 1])

    pl.semaphore_wait(barrier, sum(exists.astype(jnp.int32) for exists, _ in neighbours))

    tile_lanes = 4 * rows
    low_half = lax.broadcasted_iota(jnp.int32, (rows, 2 * tile_lanes), 1) < tile_lanes
    lane_head = (
        lax.broadcasted_iota(jnp.int32, (QUERY_COLS * rows, GROUP_FEATURES), 1) // HEAD_DIM
    )

    def build_bias(g):
        step = step_ref[...]
        masked = jnp.full(step.shape, MASKED, jnp.float32)

        def one(n, carry):
            h, x = n // BIAS_STEPS, n % BIAS_STEPS
            entry = (g * GROUP + h) * WINDOW * TABLE_STEPS + x
            tile = masked
            for a in range(WINDOW):
                value = jnp.where(
                    low_half,
                    bias_ref[entry + a * TABLE_STEPS],
                    bias_ref[entry + a * TABLE_STEPS + 1],
                )
                tile = jnp.where(step == a, value, tile)
            tile_ref[0, n] = tile
            tile_ref[1, n] = jnp.where(low_half, tile, masked)
            tile_ref[2, n] = jnp.where(low_half, masked, tile)
            tile_ref[3, n] = masked
            return carry

        lax.fori_loop(0, GROUP * BIAS_STEPS, one, 0)

    def unpack_edges(g):
        spread = spread_ref[...]
        for which in range(2):
            packed = edge_refs[g][which].reshape(-1, GROUP_FEATURES)
            wide = jnp.dot(spread, packed, preferred_element_type=jnp.float32)
            kv_refs[g][which, :, 3 * rows :, :] = wide.astype(jnp.bfloat16).reshape(
                cols + 2 * HALO, rows, GROUP_FEATURES
            )

    def attend(g):
        kv = kv_refs[g]
        features = slice(g * GROUP_FEATURES, (g + 1) * GROUP_FEATURES)

        def one(p, carry):
            at = p * ENTRY
            query = jnp.concatenate(
                [query_ref[table_ref[at + t], :, features] for t in range(QUERY_COLS)], axis=0
            )
            zero = jnp.zeros_like(query)
            stacked = jnp.concatenate(
                [jnp.where(lane_head == h, query, zero) for h in range(GROUP)], axis=0
            )
            scores = []
            per = 4
            for k in range(SLOTS // per):
                keys = jnp.concatenate(
                    [
                        kv[0, table_ref[at + QUERY_COLS + k * per + s]]
                        for s in range(per)
                    ],
                    axis=0,
                )
                score = lax.dot_general(
                    stacked, keys, (((1,), (1,)), ((), ())), preferred_element_type=jnp.float32
                )
                biases = []
                for pair in range(k * per // 2, (k + 1) * per // 2):
                    kind = table_ref[at + QUERY_COLS + SLOTS + pair]
                    biases.append(
                        jnp.concatenate(
                            [
                                tile_ref[kind, h * BIAS_STEPS + 2 * pair - t + QUERY_COLS - 1]
                                for h in range(GROUP)
                                for t in range(QUERY_COLS)
                            ],
                            axis=0,
                        )
                    )
                scores.append(score + jnp.concatenate(biases, axis=1))
            peak = functools.reduce(jnp.maximum, scores)
            peak = jnp.max(peak, axis=1, keepdims=True)
            summed, total = None, None
            for k in range(SLOTS // per):
                weight = jnp.exp(scores[k] - peak)
                values = jnp.concatenate(
                    [
                        kv[1, table_ref[at + QUERY_COLS + k * per + s]]
                        for s in range(per)
                    ],
                    axis=0,
                )
                part = jnp.dot(
                    weight.astype(jnp.bfloat16), values, preferred_element_type=jnp.float32
                )
                summed = part if summed is None else summed + part
                total = weight if total is None else total + weight
            total = jnp.sum(total, axis=1, keepdims=True)
            summed = summed / total
            tall = QUERY_COLS * rows
            result = summed[:tall]
            for h in range(1, GROUP):
                result = jnp.where(lane_head == h, summed[h * tall : (h + 1) * tall], result)
            done_ref[pl.ds(p * QUERY_COLS, QUERY_COLS)] = result.astype(jnp.bfloat16).reshape(
                QUERY_COLS, rows, GROUP_FEATURES
            )
            return carry

        lax.fori_loop(0, block_count(cols), one, 0)

        def place(j, carry):
            out_ref[j, :, features] = done_ref[slot_ref[j]]
            return carry

        lax.fori_loop(0, cols, place, 0)

    start(0, first)
    if groups > 1:
        start(1, first)
    build_bias(0)
    arrive(0, first)
    start(0, second)
    if groups > 2:
        start(2, first)
    for g in range(groups):
        if g > 0:
            build_bias(g)
        if g + 1 < groups:
            arrive(g + 1, first)
            start(g + 1, second)
            if g + 3 < groups:
                start(g + 3, first)
        arrive(g, second)
        own_copy(g).wait()
        unpack_edges(g)
        attend(g)
    for g in range(groups):
        for which in range(COPIES):
            @pl.when(sends[which])
            def _():
                copy(g, which).wait_send()


def fused_attention(table, slots, bias, step, spread, query, kv, edges):
    groups, _, cols, rows, _ = kv.shape
    span = cols + 2 * HALO
    wide = edges.shape[3] + 2 * (-(-(HALO - rows) * HALO // 16) * 16)
    smem = pl.BlockSpec(memory_space=pltpu.SMEM)
    vmem = pl.BlockSpec(memory_space=pltpu.VMEM)
    hbm = pl.BlockSpec(memory_space=pl.ANY)
    blocks = block_count(cols)
    return pl.pallas_call(
        functools.partial(fused_kernel, groups, rows, cols),
        in_specs=[smem, smem, smem, vmem, vmem, vmem, hbm, hbm],
        out_specs=vmem,
        out_shape=jax.ShapeDtypeStruct(query.shape, jnp.bfloat16),
        scratch_shapes=[
            *[pltpu.VMEM((2, span, 4 * rows, GROUP_FEATURES), jnp.bfloat16)] * groups,
            *[pltpu.VMEM((2, 2, wide, GROUP_FEATURES), jnp.bfloat16)] * groups,
            pltpu.VMEM((4, GROUP * BIAS_STEPS, rows, 8 * rows), jnp.float32),
            pltpu.VMEM((blocks * QUERY_COLS, rows, GROUP_FEATURES), jnp.bfloat16),
            pltpu.SemaphoreType.DMA((groups, COPIES)),
            pltpu.SemaphoreType.DMA((groups, COPIES)),
            pltpu.SemaphoreType.DMA((groups,)),
        ],
        compiler_params=pltpu.CompilerParams(
            collective_id=0, has_side_effects=True, vmem_limit_bytes=60 * 1024 * 1024
        ),
        cost_estimate=pl.CostEstimate(
            flops=groups * blocks * 4 * 256 * 1024 * 256,
            bytes_accessed=kv.size * 8,
            transcendentals=groups * blocks * 256 * 1024,
        ),
    )(table, slots, bias, step, spread, query, kv, edges)


def block_tables(dilation, rows, cols):
    total_cols = cols * lax.axis_size("col")
    anchor = lax.axis_index("col") * cols
    span = cols + 2 * HALO
    per_class = -(-(-(-cols // dilation)) // QUERY_COLS)
    block = jnp.arange(block_count(cols), dtype=jnp.int32)
    base = block // per_class + (block % per_class) * QUERY_COLS * dilation
    base = base[:, None]
    query_cols = jnp.clip(
        base + jnp.arange(QUERY_COLS, dtype=jnp.int32)[None] * dilation, 0, cols - 1
    )
    key_cols = base + (jnp.arange(SLOTS, dtype=jnp.int32)[None] - RADIUS_MAX) * dilation
    real = (key_cols + anchor >= 0) & (key_cols + anchor < total_cols)
    low, high = real[:, 0::2], real[:, 1::2]
    kind = jnp.where(low, jnp.where(high, 0, 1), jnp.where(high, 2, 3))
    key_cols = jnp.clip(key_cols + HALO, 0, span - 1)
    table = jnp.concatenate([query_cols, key_cols, kind], axis=1).astype(jnp.int32)
    j = jnp.arange(cols, dtype=jnp.int32)
    place = j // dilation
    slots = (j % dilation * per_class + place // QUERY_COLS) * QUERY_COLS + place % QUERY_COLS
    return table.reshape(-1), slots.astype(jnp.int32)


def bias_tables(rel_bias, pattern, radius, dilation, rows):
    total_rows = rows * lax.axis_size("row")
    anchor = lax.axis_index("row") * rows
    steps = jnp.arange(WINDOW, dtype=jnp.int32) - RADIUS_MAX
    chosen = (pattern == 1) | ((steps[:, None] == 0) & (steps[None, :] == 0))
    chosen = chosen & (jnp.abs(steps)[:, None] <= radius) & (jnp.abs(steps)[None, :] <= radius)
    bias = jnp.where(chosen[None], rel_bias, MASKED)
    before = QUERY_COLS - 1
    bias = jnp.pad(
        bias, ((0, 0), (0, 0), (before, TABLE_STEPS - WINDOW - before)), constant_values=MASKED
    )
    spill = HALO - rows
    i = lax.broadcasted_iota(jnp.int32, (rows, 8 * rows), 0)
    spot = lax.broadcasted_iota(jnp.int32, (rows, 8 * rows), 1) % (4 * rows)
    extra = spot - 3 * rows
    offset = jnp.where(
        spot < rows,
        spot,
        jnp.where(
            spot < 2 * rows,
            spot - 2 * rows,
            jnp.where(
                spot < 3 * rows,
                spot - rows,
                jnp.where(extra < spill, extra - HALO, extra - spill + 2 * rows),
            ),
        ),
    )
    real = (extra < 2 * spill) & (offset + anchor >= 0) & (offset + anchor < total_rows)
    far = offset - i
    hit = real & (far % dilation == 0) & (jnp.abs(far) <= RADIUS_MAX * dilation)
    step = jnp.where(hit, far // dilation + RADIUS_MAX, -1)
    return bias.reshape(-1), step.astype(jnp.int32)


def edge_spread(rows, cols):
    spill = HALO - rows
    span = cols + 2 * HALO
    edge = spill * cols
    side = -(-spill * HALO // 16) * 16
    wide = edge + 2 * side
    kept = side // spill
    target = lax.broadcasted_iota(jnp.int32, (span * rows, 2 * wide), 0)
    packed = lax.broadcasted_iota(jnp.int32, (span * rows, 2 * wide), 1)
    at, extra = target // rows, target % rows
    near, place = packed // wide, packed % wide
    column, line = place // spill, place % spill
    column = jnp.where(
        place < edge,
        column + HALO,
        jnp.where(
            place < edge + side,
            column - cols + HALO - kept,
            column - cols - kept + HALO + cols,
        ),
    )
    hit = (at == column) & (extra == near * spill + line)
    return hit.astype(jnp.bfloat16)


def shards(
    query_map, key_map, value_map, window_mask, tile_radius, dilation_per_tile, rel_bias, out_weight
):
    rows, cols, features = query_map.shape
    groups = features // GROUP_FEATURES
    spill = HALO - rows
    dilation = dilation_per_tile[0, 0]
    table, slots = block_tables(dilation, rows, cols)
    bias, step = bias_tables(rel_bias, window_mask[0, 0], tile_radius[0, 0], dilation, rows)

    pair = jnp.stack([key_map, value_map]).reshape(2, rows, cols, groups, GROUP_FEATURES)
    kv = pair.transpose(3, 0, 2, 1, 4)
    ends = jnp.stack([pair[:, :spill], pair[:, rows - spill :]])
    edges = ends.transpose(4, 1, 0, 3, 2, 5).reshape(
        groups, 2, 2, cols * spill, GROUP_FEATURES
    )
    query = query_map.transpose(1, 0, 2) * jnp.bfloat16(1.0 / math.sqrt(HEAD_DIM))
    attended = fused_attention(
        table, slots, bias, step, edge_spread(rows, cols), query, kv, edges
    ).reshape(cols * rows, features)

    count = lax.axis_size("head")
    model = out_weight.shape[1]
    if count != 2:
        partials = jnp.dot(attended, out_weight, preferred_element_type=jnp.float32)
        mixed = lax.psum_scatter(partials, "head", scatter_dimension=1, tiled=True)
        mixed = mixed.astype(jnp.bfloat16).reshape(cols, rows, model // count)
        return mixed.transpose(1, 0, 2)
    me = lax.axis_index("head")
    half = model // 2
    theirs = lax.dynamic_slice_in_dim(out_weight, (1 - me) * half, half, 1)
    mine = lax.dynamic_slice_in_dim(out_weight, me * half, half, 1)
    mixed = []
    parts = 2
    tokens = rows * cols // parts
    for part in range(parts):
        block = attended[part * tokens : (part + 1) * tokens]
        sent = jnp.dot(block, theirs, preferred_element_type=jnp.float32).astype(jnp.bfloat16)
        got = lax.ppermute(sent, "head", [(0, 1), (1, 0)])
        kept = jnp.dot(block, mine, preferred_element_type=jnp.float32)
        mixed.append((kept + got.astype(jnp.float32)).astype(jnp.bfloat16))
    return jnp.concatenate(mixed).reshape(cols, rows, half).transpose(1, 0, 2)


def solution(mesh):
    placed = (
        P("row", "col", "head"),
        P("row", "col", "head"),
        P("row", "col", "head"),
        P("row", "col", None, None),
        P("row", "col"),
        P("row", "col"),
        P("head", None, None),
        P("head", None),
    )
    return jax.shard_map(
        shards, mesh=mesh, in_specs=placed, out_specs=P("row", "col", "head"), check_vma=False
    )
```

```python
import functools
import math

import jax
import jax.numpy as jnp
from jax import lax
from jax.experimental import pallas as pl
from jax.experimental.pallas import tpu as pltpu
from jax.sharding import PartitionSpec as P

HEAD_DIM = 64
RADIUS_MAX = 6
DILATION_LIMIT = 3
WINDOW = 2 * RADIUS_MAX + 1
HALO = RADIUS_MAX * DILATION_LIMIT
GROUP = 4
GROUP_FEATURES = GROUP * HEAD_DIM
MASKED = -1e30

QUERY_COLS = 4
SLOTS = QUERY_COLS + WINDOW - 1
PAIRS = SLOTS // 2
BIAS_STEPS = SLOTS + QUERY_COLS - 2
TABLE_STEPS = BIAS_STEPS + 1
ENTRY = QUERY_COLS + SLOTS + PAIRS

TO_LEFT, TO_RIGHT, TO_ABOVE, TO_BELOW, TOP_UP, BOTTOM_DOWN = range(6)
MATE_LEFT, MATE_RIGHT, ACROSS_LEFT, ACROSS_RIGHT = range(6, 10)
UP_LEFT, UP_RIGHT, DOWN_LEFT, DOWN_RIGHT = range(10, 14)
COPIES = 14
SWAP, SWAP_MATE, SWAP_ACROSS, SWAP_LAST = range(4)
SWAPS = 4
TILE_KEYS = 256
LEAD, TRAIL = 2, 2


def block_count(cols):
    return max(
        d * -(-(-(-cols // d)) // QUERY_COLS) for d in range(1, DILATION_LIMIT + 1)
    )


def fused_kernel(
    groups, rows, cols, table_ref, bias_ref, step_ref, slot_ref, query_ref, key_ref, value_ref,
    weight_hbm, out_ref, *scratch
):
    kv_refs, edge_refs = scratch[:groups], scratch[groups : 2 * groups]
    (
        end_ref, tile_ref, score_a, score_b, weight_a, weight_b, total_a, total_b, turned_ref,
        done_ref, swap_ref, place_ref, spread_ref, own_ref, other_ref, mine_ref, theirs_ref,
        sum_ref, send_sems, recv_sems, swap_send, swap_recv, head_send, head_recv, own_sem,
    ) = scratch[2 * groups :]
    score_refs, weight_refs, total_refs = (score_a, score_b), (weight_a, weight_b), (total_a, total_b)
    spill = HALO - rows
    own = slice(HALO, HALO + cols)
    left, right = slice(0, HALO), slice(HALO + cols, cols + 2 * HALO)
    row, col = lax.axis_index("row"), lax.axis_index("col")
    n_row, n_col = lax.axis_size("row"), lax.axis_size("col")
    lower = lax.rem(row, 2)
    mate = row + 1 - 2 * lower
    has_left, has_right = col > 0, col < n_col - 1
    has_above, has_below = row > 0, row < n_row - 1
    has_above2, has_below2 = row > 1, row < n_row - 2
    has_mate = mate < n_row
    has_across = jnp.where(lower == 1, has_below, has_above)
    mate_rows = pl.ds(pl.multiple_of((1 + lower) * rows, rows), rows)
    across_rows = pl.ds(pl.multiple_of((1 + lower) * rows, rows), rows)
    edge = spill * cols
    side = -(-spill * HALO // 16) * 16

    def copy(g, which):
        kv, extra = kv_refs[g], edge_refs[g]
        base = slice(0, rows)
        up, down = slice(rows, 2 * rows), slice(2 * rows, 3 * rows)
        near_left, near_right = slice(HALO, 2 * HALO), slice(cols, cols + HALO)
        source, target, there = {
            TO_LEFT: (kv.at[:, near_left, base], kv.at[:, right, base], {"col": col - 1}),
            TO_RIGHT: (kv.at[:, near_right, base], kv.at[:, left, base], {"col": col + 1}),
            TO_ABOVE: (kv.at[:, own, base], kv.at[:, own, down], {"row": row - 1}),
            TO_BELOW: (kv.at[:, own, base], kv.at[:, own, up], {"row": row + 1}),
            TOP_UP: (end_ref.at[g, :, 0], extra.at[:, 1, :edge], {"row": row - 2}),
            BOTTOM_DOWN: (end_ref.at[g, :, 1], extra.at[:, 0, :edge], {"row": row + 2}),
            MATE_LEFT: (kv.at[:, left, base], kv.at[:, left, mate_rows], {"row": mate}),
            MATE_RIGHT: (kv.at[:, right, base], kv.at[:, right, mate_rows], {"row": mate}),
            ACROSS_LEFT: (
                kv.at[:, near_left, across_rows], kv.at[:, right, across_rows], {"col": col - 1}
            ),
            ACROSS_RIGHT: (
                kv.at[:, near_right, across_rows], kv.at[:, left, across_rows], {"col": col + 1}
            ),
            UP_LEFT: (
                extra.at[:, 0, :side], extra.at[:, 0, edge + side : edge + 2 * side], {"col": col - 1}
            ),
            UP_RIGHT: (
                extra.at[:, 0, edge - side : edge], extra.at[:, 0, edge : edge + side], {"col": col + 1}
            ),
            DOWN_LEFT: (
                extra.at[:, 1, :side], extra.at[:, 1, edge + side : edge + 2 * side], {"col": col - 1}
            ),
            DOWN_RIGHT: (
                extra.at[:, 1, edge - side : edge], extra.at[:, 1, edge : edge + side], {"col": col + 1}
            ),
        }[which]
        return pltpu.make_async_remote_copy(
            src_ref=source, dst_ref=target, send_sem=send_sems.at[g, which],
            recv_sem=recv_sems.at[g, which], device_id=there,
            device_id_type=pl.DeviceIdType.MESH,
        )

    sends = {
        TO_LEFT: has_left, TO_RIGHT: has_right, TO_ABOVE: has_above, TO_BELOW: has_below,
        TOP_UP: has_above2, BOTTOM_DOWN: has_below2,
        MATE_LEFT: has_mate & has_left, MATE_RIGHT: has_mate & has_right,
        ACROSS_LEFT: has_across & has_left, ACROSS_RIGHT: has_across & has_right,
        UP_LEFT: has_above2 & has_left, UP_RIGHT: has_above2 & has_right,
        DOWN_LEFT: has_below2 & has_left, DOWN_RIGHT: has_below2 & has_right,
    }
    receives = {
        TO_LEFT: has_right, TO_RIGHT: has_left, TO_ABOVE: has_below, TO_BELOW: has_above,
        TOP_UP: has_below2, BOTTOM_DOWN: has_above2,
        MATE_LEFT: has_mate & has_left, MATE_RIGHT: has_mate & has_right,
        ACROSS_LEFT: has_across & has_right, ACROSS_RIGHT: has_across & has_left,
        UP_LEFT: has_above2 & has_right, UP_RIGHT: has_above2 & has_left,
        DOWN_LEFT: has_below2 & has_right, DOWN_RIGHT: has_below2 & has_left,
    }
    first, second = tuple(range(6)), tuple(range(6, COPIES))

    def start(g, kinds):
        for which in kinds:
            @pl.when(sends[which])
            def _():
                copy(g, which).start()

    def arrive(g, kinds):
        for which in kinds:
            @pl.when(receives[which])
            def _():
                copy(g, which).wait_recv()

    head = lax.axis_index("head")
    half = out_ref.shape[1]
    quarter = theirs_ref.shape[0] // 4
    paired = row + 2 - 4 * lax.rem(row // 2, 2)
    mine = pl.ds(pl.multiple_of(lax.rem(row, 4) * quarter, quarter), quarter)
    passed = pl.ds(pl.multiple_of(lax.rem(paired, 4) * quarter, quarter), quarter)
    there_cols = pl.ds(pl.multiple_of((1 - head) * half, half), half)
    own_weight = pltpu.make_async_copy(
        weight_hbm.at[:, pl.ds(pl.multiple_of(head * half, half), half)], mine_ref, own_sem
    )

    def swap_copy(which):
        source, target, there = {
            SWAP: (weight_hbm.at[mine, there_cols], theirs_ref.at[mine], {"head": 1 - head}),
            SWAP_MATE: (theirs_ref.at[mine], theirs_ref.at[mine], {"row": mate}),
            SWAP_ACROSS: (theirs_ref.at[mine], theirs_ref.at[mine], {"row": paired}),
            SWAP_LAST: (theirs_ref.at[passed], theirs_ref.at[passed], {"row": mate}),
        }[which]
        return pltpu.make_async_remote_copy(
            src_ref=source, dst_ref=target, send_sem=swap_send.at[which],
            recv_sem=swap_recv.at[which], device_id=there,
            device_id_type=pl.DeviceIdType.MESH,
        )

    def head_copy(g):
        return pltpu.make_async_remote_copy(
            src_ref=own_ref.at[g], dst_ref=other_ref.at[g], send_sem=head_send.at[g],
            recv_sem=head_recv.at[g], device_id={"head": 1 - head},
            device_id_type=pl.DeviceIdType.MESH,
        )

    neighbours = (
        (has_left, {"col": col - 1}), (has_right, {"col": col + 1}),
        (has_above, {"row": row - 1}), (has_below, {"row": row + 1}),
        (has_above2, {"row": row - 2}), (has_below2, {"row": row + 2}),
        (head >= 0, {"head": 1 - head}),
    )
    barrier = pltpu.get_barrier_semaphore()
    for exists, there in neighbours:
        @pl.when(exists)
        def _():
            pl.semaphore_signal(
                barrier, inc=1, device_id=there, device_id_type=pl.DeviceIdType.MESH
            )
    own_weight.start()

    def clear(part):
        part[...] = jnp.zeros(part.shape, part.dtype)

    for g in range(groups):
        kv, extra = kv_refs[g], edge_refs[g]
        for which in range(2):
            @pl.when(jnp.logical_not(has_left))
            def _():
                clear(kv.at[which, left, : 3 * rows])
                for near in range(2):
                    clear(extra.at[which, near, edge : edge + side])

            @pl.when(jnp.logical_not(has_right))
            def _():
                clear(kv.at[which, right, : 3 * rows])
                for near in range(2):
                    clear(extra.at[which, near, edge + side :])

            @pl.when(jnp.logical_not(has_above))
            def _():
                clear(kv.at[which, :, rows : 2 * rows])

            @pl.when(jnp.logical_not(has_below))
            def _():
                clear(kv.at[which, :, 2 * rows : 3 * rows])

            @pl.when(jnp.logical_not(has_above2))
            def _():
                clear(extra.at[which, 0])

            @pl.when(jnp.logical_not(has_below2))
            def _():
                clear(extra.at[which, 1])

    def iota(shape, axis):
        return lax.broadcasted_iota(jnp.int32, shape, axis)

    tokens = rows * cols
    place, source = iota((tokens, tokens), 0), iota((tokens, tokens), 1)
    swap_ref[:tokens] = (source == place % rows * cols + place // rows).astype(
        jnp.float32
    ).astype(jnp.bfloat16)
    place, source = iota((2 * edge, tokens), 0), iota((2 * edge, tokens), 1)
    line = place % edge % spill + jnp.where(place < edge, 0, rows - spill)
    swap_ref[tokens:] = (source == line * cols + place % edge // spill).astype(
        jnp.float32
    ).astype(jnp.bfloat16)

    def turn(g):
        features = slice(g * GROUP_FEATURES, (g + 1) * GROUP_FEATURES)
        for which, ref in ((0, key_ref), (1, value_ref)):
            moved = jnp.dot(
                swap_ref[...], ref[:, :, features].reshape(-1, GROUP_FEATURES),
                preferred_element_type=jnp.float32,
            ).astype(jnp.bfloat16)
            kv_refs[g][which, own, :rows] = moved[:tokens].reshape(cols, rows, GROUP_FEATURES)
            end_ref[g, which] = moved[tokens:].reshape(2, edge, GROUP_FEATURES)

    turn(0)
    if groups > 1:
        turn(1)
    pl.semaphore_wait(barrier, sum(exists.astype(jnp.int32) for exists, _ in neighbours))

    tile_lanes = 4 * rows
    low_half = lax.broadcasted_iota(jnp.int32, (rows, 2 * tile_lanes), 1) < tile_lanes
    lane_head = (
        lax.broadcasted_iota(jnp.int32, (QUERY_COLS * rows, GROUP_FEATURES), 1) // HEAD_DIM
    )

    def build_bias(g):
        step = step_ref[...]
        masked = jnp.full(step.shape, MASKED, jnp.float32)

        def one(n, carry):
            h, x = n // BIAS_STEPS, n % BIAS_STEPS
            entry = (g * GROUP + h) * WINDOW * TABLE_STEPS + x
            tile = masked
            for a in range(WINDOW):
                value = jnp.where(
                    low_half,
                    bias_ref[entry + a * TABLE_STEPS],
                    bias_ref[entry + a * TABLE_STEPS + 1],
                )
                tile = jnp.where(step == a, value, tile)
            tile_ref[0, n] = tile
            tile_ref[1, n] = jnp.where(low_half, tile, masked)
            tile_ref[2, n] = jnp.where(low_half, masked, tile)
            tile_ref[3, n] = masked
            return carry

        lax.fori_loop(0, GROUP * BIAS_STEPS, one, 0)

    def unpack_edges(g):
        spread = spread_ref[...]
        for which in range(2):
            packed = edge_refs[g][which].reshape(-1, GROUP_FEATURES)
            wide = jnp.dot(spread, packed, preferred_element_type=jnp.float32)
            kv_refs[g][which, :, 3 * rows :, :] = wide.astype(jnp.bfloat16).reshape(
                cols + 2 * HALO, rows, GROUP_FEATURES
            )

    def attend(g):
        kv = kv_refs[g]
        features = slice(g * GROUP_FEATURES, (g + 1) * GROUP_FEATURES)
        near = TILE_KEYS // (4 * rows)
        tall = QUERY_COLS * rows
        blocks = block_count(cols)
        turned = jnp.dot(
            swap_ref[: rows * cols], query_ref[:, :, features].reshape(-1, GROUP_FEATURES),
            preferred_element_type=jnp.float32,
        ) * (1.0 / math.sqrt(HEAD_DIM))
        turned_ref[...] = turned.astype(jnp.bfloat16).reshape(cols, rows, GROUP_FEATURES)

        def keys_at(p, which, k):
            at = p * ENTRY + QUERY_COLS + k * near
            return jnp.concatenate(
                [kv[which, table_ref[at + s]] for s in range(near)], axis=0
            )

        def multiply(p, score_ref):
            query = jnp.concatenate(
                [turned_ref[table_ref[p * ENTRY + t]] for t in range(QUERY_COLS)], axis=0
            )
            zero = jnp.zeros_like(query)
            stacked = jnp.concatenate(
                [jnp.where(lane_head == h, query, zero) for h in range(GROUP)], axis=0
            )
            for k in range(SLOTS // near):
                score_ref[:, k * TILE_KEYS : (k + 1) * TILE_KEYS] = lax.dot_general(
                    stacked, keys_at(p, 0, k), (((1,), (1,)), ((), ())),
                    preferred_element_type=jnp.float32,
                )

        def soften(p, score_ref, weight_ref, total_ref):
            at = p * ENTRY + QUERY_COLS + SLOTS
            kinds = [table_ref[at + pair] for pair in range(PAIRS)]
            lanes = 8 * rows
            for h in range(GROUP):
                for t in range(QUERY_COLS):
                    here = slice((h * QUERY_COLS + t) * rows, (h * QUERY_COLS + t + 1) * rows)
                    parts = [
                        score_ref[here, pair * lanes : (pair + 1) * lanes]
                        + tile_ref[kinds[pair], h * BIAS_STEPS + 2 * pair - t + QUERY_COLS - 1]
                        for pair in range(PAIRS)
                    ]
                    peak = jnp.max(functools.reduce(jnp.maximum, parts), axis=1, keepdims=True)
                    parts = [jnp.exp(part - peak) for part in parts]
                    total = jnp.sum(functools.reduce(jnp.add, parts), axis=1, keepdims=True)
                    for pair in range(PAIRS):
                        weight_ref[here, pair * lanes : (pair + 1) * lanes] = parts[pair].astype(
                            jnp.bfloat16
                        )
                    total_ref[here] = jnp.broadcast_to(total, (rows, GROUP_FEATURES // 2))

        def finish(p, weight_ref, total_ref):
            values = jnp.concatenate(
                [keys_at(p, 1, k) for k in range(SLOTS // near)], axis=0
            )
            summed = jnp.dot(weight_ref[...], values, preferred_element_type=jnp.float32)
            result = summed[:tall]
            total = total_ref[...]
            total = jnp.concatenate([total, total], axis=1)
            share = total[:tall]
            for h in range(1, GROUP):
                part = slice(h * tall, (h + 1) * tall)
                result = jnp.where(lane_head == h, summed[part], result)
                share = jnp.where(lane_head == h, total[part], share)
            row_at = p * tall if isinstance(p, int) else pl.multiple_of(p * tall, tall)
            done_ref[pl.ds(row_at, tall)] = (result / share).astype(
                jnp.bfloat16
            )

        def two(n, carry):
            for side in range(2):
                i = 2 * n + side
                finish(i, weight_refs[side], total_refs[side])
                soften(
                    i + 1, score_refs[1 - side], weight_refs[1 - side], total_refs[1 - side]
                )
                multiply(i + 2, score_refs[side])
            return carry

        steps = blocks + 1
        lax.fori_loop(0, -(-steps // 2), two, 0)
        if steps % 2 == 0:
            finish(LEAD + blocks - 1, weight_refs[(blocks - 1) % 2], total_refs[(blocks - 1) % 2])

        own_ref[g] = jnp.dot(
            place_ref[...], done_ref[LEAD * tall :], preferred_element_type=jnp.float32
        ).astype(jnp.bfloat16)

    start(0, first)
    swap_copy(SWAP).start()
    if groups > 1:
        start(1, first)
    span = cols + 2 * HALO
    wide = spread_ref.shape[1] // 2
    kept = side // spill
    target, packed = iota(spread_ref.shape, 0), iota(spread_ref.shape, 1)
    at, line = target // rows, target % rows
    second_half = packed >= wide
    spot = packed - jnp.where(second_half, wide, 0)
    column = spot // spill
    column = jnp.where(
        spot < edge,
        column + HALO,
        jnp.where(spot < edge + side, column - cols + HALO - kept, column - kept + HALO),
    )
    wanted = jnp.where(second_half, spill, 0) + spot % spill
    spread_ref[...] = ((at == column) & (line == wanted)).astype(jnp.float32).astype(jnp.bfloat16)
    place_ref[...] = (
        iota(place_ref.shape, 1) == jnp.broadcast_to(slot_ref[...], place_ref.shape)
    ).astype(jnp.float32).astype(jnp.bfloat16)
    for g in range(2, groups):
        turn(g)
    build_bias(0)
    arrive(0, first)
    start(0, second)
    if groups > 2:
        start(2, first)

    model_tiles = half // GROUP_FEATURES

    def project(g):
        weights = slice(g * GROUP_FEATURES, (g + 1) * GROUP_FEATURES)

        def one(n, carry):
            lanes = pl.ds(pl.multiple_of(n * GROUP_FEATURES, GROUP_FEATURES), GROUP_FEATURES)
            part = jnp.dot(own_ref[g], mine_ref[weights, lanes], preferred_element_type=jnp.float32)
            sum_ref[:, lanes] = part if g == 0 else sum_ref[:, lanes] + part
            return carry

        lax.fori_loop(0, model_tiles, one, 0)

    pass_on, pass_last = min(2, groups - 1), min(4, groups - 1)
    for g in range(groups):
        if g > 0:
            head_copy(g - 1).start()
            build_bias(g)
        if g + 1 < groups:
            arrive(g + 1, first)
            start(g + 1, second)
            if g + 3 < groups:
                start(g + 3, first)
        if g == pass_on:
            swap_copy(SWAP).wait_recv()
            swap_copy(SWAP_ACROSS).start()
            swap_copy(SWAP_MATE).start()
        if g == pass_last:
            swap_copy(SWAP_ACROSS).wait_recv()
            swap_copy(SWAP_LAST).start()
        arrive(g, second)
        unpack_edges(g)
        attend(g)
        if g == 0:
            own_weight.wait()
        project(g)
    head_copy(groups - 1).start()
    swap_copy(SWAP_MATE).wait_recv()
    swap_copy(SWAP_LAST).wait_recv()
    for g in range(groups):
        head_copy(g).wait_recv()

    def last(n, carry):
        lanes = pl.ds(pl.multiple_of(n * GROUP_FEATURES, GROUP_FEATURES), GROUP_FEATURES)
        total = sum_ref[:, lanes]
        for g in range(groups):
            weights = slice(g * GROUP_FEATURES, (g + 1) * GROUP_FEATURES)
            total = total + jnp.dot(
                other_ref[g], theirs_ref[weights, lanes], preferred_element_type=jnp.float32
            )
        out_ref[:, lanes] = total.astype(jnp.bfloat16)
        return carry

    lax.fori_loop(0, model_tiles, last, 0)
    for g in range(groups):
        for which in range(COPIES):
            @pl.when(sends[which])
            def _():
                copy(g, which).wait_send()
        head_copy(g).wait_send()
    for which in range(SWAPS):
        swap_copy(which).wait_send()


def fused_layer(table, bias, step, slots, query, key, value, weight):
    rows, cols, features = query.shape
    groups = features // GROUP_FEATURES
    tokens = rows * cols
    half = weight.shape[1] // 2
    span = cols + 2 * HALO
    spill = HALO - rows
    edge = spill * cols
    wide = edge + 2 * (-(-spill * HALO // 16) * 16)
    smem = pl.BlockSpec(memory_space=pltpu.SMEM)
    vmem = pl.BlockSpec(memory_space=pltpu.VMEM)
    hbm = pl.BlockSpec(memory_space=pl.ANY)
    blocks = block_count(cols)
    stacked = GROUP * QUERY_COLS * rows
    keys = SLOTS * 4 * rows
    half_type = jnp.bfloat16
    return pl.pallas_call(
        functools.partial(fused_kernel, groups, rows, cols),
        in_specs=[smem, smem, vmem, vmem, vmem, vmem, vmem, hbm],
        out_specs=vmem,
        out_shape=jax.ShapeDtypeStruct((tokens, half), half_type),
        scratch_shapes=[
            *[pltpu.VMEM((2, span, 4 * rows, GROUP_FEATURES), half_type)] * groups,
            *[pltpu.VMEM((2, 2, wide, GROUP_FEATURES), half_type)] * groups,
            pltpu.VMEM((groups, 2, 2, edge, GROUP_FEATURES), half_type),
            pltpu.VMEM((4, GROUP * BIAS_STEPS, rows, 8 * rows), jnp.float32),
            pltpu.VMEM((stacked, keys), jnp.float32),
            pltpu.VMEM((stacked, keys), jnp.float32),
            pltpu.VMEM((stacked, keys), half_type),
            pltpu.VMEM((stacked, keys), half_type),
            pltpu.VMEM((stacked, GROUP_FEATURES // 2), jnp.float32),
            pltpu.VMEM((stacked, GROUP_FEATURES // 2), jnp.float32),
            pltpu.VMEM((cols, rows, GROUP_FEATURES), half_type),
            pltpu.VMEM(((LEAD + blocks) * QUERY_COLS * rows, GROUP_FEATURES), half_type),
            pltpu.VMEM((tokens + 2 * edge, tokens), half_type),
            pltpu.VMEM((tokens, blocks * QUERY_COLS * rows), half_type),
            pltpu.VMEM((span * rows, 2 * wide), half_type),
            pltpu.VMEM((groups, tokens, GROUP_FEATURES), half_type),
            pltpu.VMEM((groups, tokens, GROUP_FEATURES), half_type),
            pltpu.VMEM((features, half), half_type),
            pltpu.VMEM((features, half), half_type),
            pltpu.VMEM((tokens, half), jnp.float32),
            pltpu.SemaphoreType.DMA((groups, COPIES)),
            pltpu.SemaphoreType.DMA((groups, COPIES)),
            pltpu.SemaphoreType.DMA((SWAPS,)),
            pltpu.SemaphoreType.DMA((SWAPS,)),
            pltpu.SemaphoreType.DMA((groups,)),
            pltpu.SemaphoreType.DMA((groups,)),
            pltpu.SemaphoreType.DMA,
        ],
        compiler_params=pltpu.CompilerParams(
            collective_id=0, has_side_effects=True, vmem_limit_bytes=67043328
        ),
        cost_estimate=pl.CostEstimate(
            flops=groups * blocks * 4 * stacked * keys * GROUP_FEATURES,
            bytes_accessed=query.size * 8,
            transcendentals=groups * blocks * stacked * keys,
        ),
    )(table, bias, step, slots, query, key, value, weight)


def block_tables(dilation, rows, cols):
    total_cols = cols * lax.axis_size("col")
    anchor = lax.axis_index("col") * cols
    span = cols + 2 * HALO
    per_class = -(-(-(-cols // dilation)) // QUERY_COLS)
    block = jnp.arange(block_count(cols), dtype=jnp.int32)
    base = block // per_class + (block % per_class) * QUERY_COLS * dilation
    base = base[:, None]
    query_cols = jnp.clip(
        base + jnp.arange(QUERY_COLS, dtype=jnp.int32)[None] * dilation, 0, cols - 1
    )
    key_cols = base + (jnp.arange(SLOTS, dtype=jnp.int32)[None] - RADIUS_MAX) * dilation
    real = (key_cols + anchor >= 0) & (key_cols + anchor < total_cols)
    low, high = real[:, 0::2], real[:, 1::2]
    kind = jnp.where(low, jnp.where(high, 0, 1), jnp.where(high, 2, 3))
    key_cols = jnp.clip(key_cols + HALO, 0, span - 1)
    table = jnp.concatenate([query_cols, key_cols, kind], axis=1).astype(jnp.int32)
    table = jnp.pad(table, ((LEAD, TRAIL), (0, 0)))
    j = jnp.arange(cols, dtype=jnp.int32)
    place = j // dilation
    slots = (j % dilation * per_class + place // QUERY_COLS) * QUERY_COLS + place % QUERY_COLS
    slots = slots[None, :] * rows + jnp.arange(rows, dtype=jnp.int32)[:, None]
    return table.reshape(-1), slots.reshape(rows * cols, 1).astype(jnp.int32)


def bias_tables(rel_bias, pattern, radius, dilation, rows):
    total_rows = rows * lax.axis_size("row")
    anchor = lax.axis_index("row") * rows
    steps = jnp.arange(WINDOW, dtype=jnp.int32) - RADIUS_MAX
    chosen = (pattern == 1) | ((steps[:, None] == 0) & (steps[None, :] == 0))
    chosen = chosen & (jnp.abs(steps)[:, None] <= radius) & (jnp.abs(steps)[None, :] <= radius)
    bias = jnp.where(chosen[None], rel_bias, MASKED)
    before = QUERY_COLS - 1
    bias = jnp.pad(
        bias, ((0, 0), (0, 0), (before, TABLE_STEPS - WINDOW - before)), constant_values=MASKED
    )
    spill = HALO - rows
    i = lax.broadcasted_iota(jnp.int32, (rows, 8 * rows), 0)
    spot = lax.broadcasted_iota(jnp.int32, (rows, 8 * rows), 1) % (4 * rows)
    extra = spot - 3 * rows
    offset = jnp.where(
        spot < rows,
        spot,
        jnp.where(
            spot < 2 * rows,
            spot - 2 * rows,
            jnp.where(
                spot < 3 * rows,
                spot - rows,
                jnp.where(extra < spill, extra - HALO, extra - spill + 2 * rows),
            ),
        ),
    )
    real = (extra < 2 * spill) & (offset + anchor >= 0) & (offset + anchor < total_rows)
    far = offset - i
    hit = real & (far % dilation == 0) & (jnp.abs(far) <= RADIUS_MAX * dilation)
    step = jnp.where(hit, far // dilation + RADIUS_MAX, -1)
    return bias.reshape(-1), step.astype(jnp.int32)


def shards(
    query_map, key_map, value_map, window_mask, tile_radius, dilation_per_tile, rel_bias, out_weight
):
    rows, cols, features = query_map.shape
    dilation = dilation_per_tile[0, 0]
    table, slots = block_tables(dilation, rows, cols)
    bias, step = bias_tables(rel_bias, window_mask[0, 0], tile_radius[0, 0], dilation, rows)
    mixed = fused_layer(
        table, bias, step, slots, query_map, key_map, value_map, out_weight
    )
    return mixed.reshape(rows, cols, out_weight.shape[1] // 2)


def solution(mesh):
    placed = (
        P("row", "col", "head"),
        P("row", "col", "head"),
        P("row", "col", "head"),
        P("row", "col", None, None),
        P("row", "col"),
        P("row", "col"),
        P("head", None, None),
        P("head", None),
    )
    return jax.shard_map(
        shards, mesh=mesh, in_specs=placed, out_specs=P("row", "col", "head"), check_vma=False
    )
```

```python
import functools
import math

import jax
import jax.numpy as jnp
from jax import lax
from jax.experimental import pallas as pl
from jax.experimental.pallas import tpu as pltpu
from jax.sharding import PartitionSpec as P

HEAD_DIM = 64
RADIUS_MAX = 6
DILATION_LIMIT = 3
WINDOW = 2 * RADIUS_MAX + 1
HALO = RADIUS_MAX * DILATION_LIMIT
GROUP = 4
GROUP_FEATURES = GROUP * HEAD_DIM
MASKED = -1e30

QUERY_COLS = 4
SLOTS = QUERY_COLS + WINDOW - 1
PAIRS = SLOTS // 2
BIAS_STEPS = SLOTS + QUERY_COLS - 2
TABLE_STEPS = BIAS_STEPS + 1
ENTRY = QUERY_COLS + SLOTS + PAIRS

TO_LEFT, TO_RIGHT, TO_ABOVE, TO_BELOW, TOP_UP, BOTTOM_DOWN = range(6)
MATE_LEFT, MATE_RIGHT, ACROSS_LEFT, ACROSS_RIGHT = range(6, 10)
UP_LEFT, UP_RIGHT, DOWN_LEFT, DOWN_RIGHT = range(10, 14)
COPIES = 14
SWAP, SWAP_MATE, SWAP_ACROSS, SWAP_LAST = range(4)
SWAPS = 4
TILE_KEYS = 256
LEAD, TRAIL = 2, 2


def block_count(cols):
    return max(
        d * -(-(-(-cols // d)) // QUERY_COLS) for d in range(1, DILATION_LIMIT + 1)
    )


def fused_kernel(
    groups, rows, cols, dilation_ref, table_ref, bias_ref, query_ref, key_ref, value_ref,
    weight_hbm, out_ref, *scratch
):
    kv_refs, edge_refs = scratch[:groups], scratch[groups : 2 * groups]
    (
        end_ref, tile_ref, score_a, score_b, weight_a, weight_b, total_a, total_b, turned_ref,
        done_ref, swap_ref, place_ref, spread_ref, own_ref, other_ref, mine_ref, theirs_ref,
        sum_ref, send_sems, recv_sems, swap_send, swap_recv, head_send, head_recv, own_sem,
    ) = scratch[2 * groups :]
    score_refs, weight_refs, total_refs = (score_a, score_b), (weight_a, weight_b), (total_a, total_b)
    spill = HALO - rows
    own = slice(HALO, HALO + cols)
    left, right = slice(0, HALO), slice(HALO + cols, cols + 2 * HALO)
    row, col = lax.axis_index("row"), lax.axis_index("col")
    n_row, n_col = lax.axis_size("row"), lax.axis_size("col")
    lower = lax.rem(row, 2)
    mate = row + 1 - 2 * lower
    has_left, has_right = col > 0, col < n_col - 1
    has_above, has_below = row > 0, row < n_row - 1
    has_above2, has_below2 = row > 1, row < n_row - 2
    has_mate = mate < n_row
    has_across = jnp.where(lower == 1, has_below, has_above)
    mate_rows = pl.ds(pl.multiple_of((1 + lower) * rows, rows), rows)
    across_rows = pl.ds(pl.multiple_of((1 + lower) * rows, rows), rows)
    edge = spill * cols
    side = -(-spill * HALO // 16) * 16

    def copy(g, which):
        kv, extra = kv_refs[g], edge_refs[g]
        base = slice(0, rows)
        up, down = slice(rows, 2 * rows), slice(2 * rows, 3 * rows)
        near_left, near_right = slice(HALO, 2 * HALO), slice(cols, cols + HALO)
        source, target, there = {
            TO_LEFT: (kv.at[:, near_left, base], kv.at[:, right, base], {"col": col - 1}),
            TO_RIGHT: (kv.at[:, near_right, base], kv.at[:, left, base], {"col": col + 1}),
            TO_ABOVE: (kv.at[:, own, base], kv.at[:, own, down], {"row": row - 1}),
            TO_BELOW: (kv.at[:, own, base], kv.at[:, own, up], {"row": row + 1}),
            TOP_UP: (end_ref.at[g, :, 0], extra.at[:, 1, :edge], {"row": row - 2}),
            BOTTOM_DOWN: (end_ref.at[g, :, 1], extra.at[:, 0, :edge], {"row": row + 2}),
            MATE_LEFT: (kv.at[:, left, base], kv.at[:, left, mate_rows], {"row": mate}),
            MATE_RIGHT: (kv.at[:, right, base], kv.at[:, right, mate_rows], {"row": mate}),
            ACROSS_LEFT: (
                kv.at[:, near_left, across_rows], kv.at[:, right, across_rows], {"col": col - 1}
            ),
            ACROSS_RIGHT: (
                kv.at[:, near_right, across_rows], kv.at[:, left, across_rows], {"col": col + 1}
            ),
            UP_LEFT: (
                extra.at[:, 0, :side], extra.at[:, 0, edge + side : edge + 2 * side], {"col": col - 1}
            ),
            UP_RIGHT: (
                extra.at[:, 0, edge - side : edge], extra.at[:, 0, edge : edge + side], {"col": col + 1}
            ),
            DOWN_LEFT: (
                extra.at[:, 1, :side], extra.at[:, 1, edge + side : edge + 2 * side], {"col": col - 1}
            ),
            DOWN_RIGHT: (
                extra.at[:, 1, edge - side : edge], extra.at[:, 1, edge : edge + side], {"col": col + 1}
            ),
        }[which]
        return pltpu.make_async_remote_copy(
            src_ref=source, dst_ref=target, send_sem=send_sems.at[g, which],
            recv_sem=recv_sems.at[g, which], device_id=there,
            device_id_type=pl.DeviceIdType.MESH,
        )

    sends = {
        TO_LEFT: has_left, TO_RIGHT: has_right, TO_ABOVE: has_above, TO_BELOW: has_below,
        TOP_UP: has_above2, BOTTOM_DOWN: has_below2,
        MATE_LEFT: has_mate & has_left, MATE_RIGHT: has_mate & has_right,
        ACROSS_LEFT: has_across & has_left, ACROSS_RIGHT: has_across & has_right,
        UP_LEFT: has_above2 & has_left, UP_RIGHT: has_above2 & has_right,
        DOWN_LEFT: has_below2 & has_left, DOWN_RIGHT: has_below2 & has_right,
    }
    receives = {
        TO_LEFT: has_right, TO_RIGHT: has_left, TO_ABOVE: has_below, TO_BELOW: has_above,
        TOP_UP: has_below2, BOTTOM_DOWN: has_above2,
        MATE_LEFT: has_mate & has_left, MATE_RIGHT: has_mate & has_right,
        ACROSS_LEFT: has_across & has_right, ACROSS_RIGHT: has_across & has_left,
        UP_LEFT: has_above2 & has_right, UP_RIGHT: has_above2 & has_left,
        DOWN_LEFT: has_below2 & has_right, DOWN_RIGHT: has_below2 & has_left,
    }
    first, second = tuple(range(6)), tuple(range(6, COPIES))

    def start(g, kinds):
        for which in kinds:
            @pl.when(sends[which])
            def _():
                copy(g, which).start()

    def arrive(g, kinds):
        for which in kinds:
            @pl.when(receives[which])
            def _():
                copy(g, which).wait_recv()

    head = lax.axis_index("head")
    half = out_ref.shape[1]
    quarter = theirs_ref.shape[0] // 4
    paired = row + 2 - 4 * lax.rem(row // 2, 2)
    mine = pl.ds(pl.multiple_of(lax.rem(row, 4) * quarter, quarter), quarter)
    passed = pl.ds(pl.multiple_of(lax.rem(paired, 4) * quarter, quarter), quarter)
    there_cols = pl.ds(pl.multiple_of((1 - head) * half, half), half)
    own_weight = pltpu.make_async_copy(
        weight_hbm.at[:, pl.ds(pl.multiple_of(head * half, half), half)], mine_ref, own_sem
    )

    def swap_copy(which):
        source, target, there = {
            SWAP: (weight_hbm.at[mine, there_cols], theirs_ref.at[mine], {"head": 1 - head}),
            SWAP_MATE: (theirs_ref.at[mine], theirs_ref.at[mine], {"row": mate}),
            SWAP_ACROSS: (theirs_ref.at[mine], theirs_ref.at[mine], {"row": paired}),
            SWAP_LAST: (theirs_ref.at[passed], theirs_ref.at[passed], {"row": mate}),
        }[which]
        return pltpu.make_async_remote_copy(
            src_ref=source, dst_ref=target, send_sem=swap_send.at[which],
            recv_sem=swap_recv.at[which], device_id=there,
            device_id_type=pl.DeviceIdType.MESH,
        )

    def head_copy(g):
        return pltpu.make_async_remote_copy(
            src_ref=own_ref.at[g], dst_ref=other_ref.at[g], send_sem=head_send.at[g],
            recv_sem=head_recv.at[g], device_id={"head": 1 - head},
            device_id_type=pl.DeviceIdType.MESH,
        )

    neighbours = (
        (has_left, {"col": col - 1}), (has_right, {"col": col + 1}),
        (has_above, {"row": row - 1}), (has_below, {"row": row + 1}),
        (has_above2, {"row": row - 2}), (has_below2, {"row": row + 2}),
        (head >= 0, {"head": 1 - head}),
    )
    barrier = pltpu.get_barrier_semaphore()
    for exists, there in neighbours:
        @pl.when(exists)
        def _():
            pl.semaphore_signal(
                barrier, inc=1, device_id=there, device_id_type=pl.DeviceIdType.MESH
            )
    own_weight.start()

    def clear(part):
        part[...] = jnp.zeros(part.shape, part.dtype)

    for g in range(groups):
        kv, extra = kv_refs[g], edge_refs[g]
        for which in range(2):
            @pl.when(jnp.logical_not(has_left))
            def _():
                clear(kv.at[which, left, : 3 * rows])
                for near in range(2):
                    clear(extra.at[which, near, edge : edge + side])

            @pl.when(jnp.logical_not(has_right))
            def _():
                clear(kv.at[which, right, : 3 * rows])
                for near in range(2):
                    clear(extra.at[which, near, edge + side :])

            @pl.when(jnp.logical_not(has_above))
            def _():
                clear(kv.at[which, :, rows : 2 * rows])

            @pl.when(jnp.logical_not(has_below))
            def _():
                clear(kv.at[which, :, 2 * rows : 3 * rows])

            @pl.when(jnp.logical_not(has_above2))
            def _():
                clear(extra.at[which, 0])

            @pl.when(jnp.logical_not(has_below2))
            def _():
                clear(extra.at[which, 1])

    def iota(shape, axis):
        return lax.broadcasted_iota(jnp.int32, shape, axis)

    tokens = rows * cols
    place, source = iota((tokens, tokens), 0), iota((tokens, tokens), 1)
    swap_ref[:tokens] = (source == place % rows * cols + place // rows).astype(
        jnp.float32
    ).astype(jnp.bfloat16)
    place, source = iota((2 * edge, tokens), 0), iota((2 * edge, tokens), 1)
    line = place % edge % spill + jnp.where(place < edge, 0, rows - spill)
    swap_ref[tokens:] = (source == line * cols + place % edge // spill).astype(
        jnp.float32
    ).astype(jnp.bfloat16)

    def turn(g):
        features = slice(g * GROUP_FEATURES, (g + 1) * GROUP_FEATURES)
        for which, ref in ((0, key_ref), (1, value_ref)):
            moved = jnp.dot(
                swap_ref[...], ref[:, :, features].reshape(-1, GROUP_FEATURES),
                preferred_element_type=jnp.float32,
            ).astype(jnp.bfloat16)
            kv_refs[g][which, own, :rows] = moved[:tokens].reshape(cols, rows, GROUP_FEATURES)
            end_ref[g, which] = moved[tokens:].reshape(2, edge, GROUP_FEATURES)

    turn(0)
    if groups > 1:
        turn(1)
    pl.semaphore_wait(barrier, sum(exists.astype(jnp.int32) for exists, _ in neighbours))

    tile_lanes = 4 * rows
    low_half = lax.broadcasted_iota(jnp.int32, (rows, 2 * tile_lanes), 1) < tile_lanes
    lane_head = (
        lax.broadcasted_iota(jnp.int32, (QUERY_COLS * rows, GROUP_FEATURES), 1) // HEAD_DIM
    )

    def by_dilation(values):
        chosen = values[DILATION_LIMIT]
        for d in range(1, DILATION_LIMIT):
            chosen = jnp.where(dilation_ref[0] == d, values[d], chosen)
        return chosen

    def window_step():
        shape = (rows, 8 * rows)
        spot = iota(shape, 1) % (4 * rows)
        extra = spot - 3 * rows
        offset = jnp.where(
            spot < rows,
            spot,
            jnp.where(
                spot < 2 * rows,
                spot - 2 * rows,
                jnp.where(
                    spot < 3 * rows,
                    spot - rows,
                    jnp.where(extra < spill, extra - HALO, extra - spill + 2 * rows),
                ),
            ),
        )
        anchor = row * rows
        real = (extra < 2 * spill) & (offset + anchor >= 0) & (offset + anchor < n_row * rows)
        far = offset - iota(shape, 0)
        lift = DILATION_LIMIT * 2 * HALO
        steps = {}
        for d in range(1, DILATION_LIMIT + 1):
            hit = ((far + lift) % d == 0) & (jnp.abs(far) <= RADIUS_MAX * d)
            steps[d] = jnp.where(hit, (far + lift) // d - lift // d + RADIUS_MAX, -1)
        return jnp.where(real, by_dilation(steps), -1)

    def column_slots(shape):
        token = iota(shape, 0)
        line, column = token // cols, token % cols
        slots = {}
        for d in range(1, DILATION_LIMIT + 1):
            per_class = -(-(-(-cols // d)) // QUERY_COLS)
            at = column // d
            slots[d] = (column % d * per_class + at // QUERY_COLS) * QUERY_COLS + at % QUERY_COLS
        return by_dilation(slots) * rows + line

    def build_bias(g):
        step = window_step()
        masked = jnp.full(step.shape, MASKED, jnp.float32)

        def one(n, carry):
            h, x = n // BIAS_STEPS, n % BIAS_STEPS
            entry = (g * GROUP + h) * WINDOW * TABLE_STEPS + x
            tile = masked
            for a in range(WINDOW):
                value = jnp.where(
                    low_half,
                    bias_ref[entry + a * TABLE_STEPS],
                    bias_ref[entry + a * TABLE_STEPS + 1],
                )
                tile = jnp.where(step == a, value, tile)
            tile_ref[0, n] = tile
            tile_ref[1, n] = jnp.where(low_half, tile, masked)
            tile_ref[2, n] = jnp.where(low_half, masked, tile)
            tile_ref[3, n] = masked
            return carry

        lax.fori_loop(0, GROUP * BIAS_STEPS, one, 0)

    def unpack_edges(g):
        spread = spread_ref[...]
        for which in range(2):
            packed = edge_refs[g][which].reshape(-1, GROUP_FEATURES)
            wide = jnp.dot(spread, packed, preferred_element_type=jnp.float32)
            kv_refs[g][which, :, 3 * rows :, :] = wide.astype(jnp.bfloat16).reshape(
                cols + 2 * HALO, rows, GROUP_FEATURES
            )

    def attend(g):
        kv = kv_refs[g]
        features = slice(g * GROUP_FEATURES, (g + 1) * GROUP_FEATURES)
        near = TILE_KEYS // (4 * rows)
        tall = QUERY_COLS * rows
        blocks = block_count(cols)
        turned = jnp.dot(
            swap_ref[: rows * cols], query_ref[:, :, features].reshape(-1, GROUP_FEATURES),
            preferred_element_type=jnp.float32,
        ) * (1.0 / math.sqrt(HEAD_DIM))
        turned_ref[...] = turned.astype(jnp.bfloat16).reshape(cols, rows, GROUP_FEATURES)

        def keys_at(p, which, k):
            at = p * ENTRY + QUERY_COLS + k * near
            return jnp.concatenate(
                [kv[which, table_ref[at + s]] for s in range(near)], axis=0
            )

        def multiply(p, score_ref):
            query = jnp.concatenate(
                [turned_ref[table_ref[p * ENTRY + t]] for t in range(QUERY_COLS)], axis=0
            )
            zero = jnp.zeros_like(query)
            stacked = jnp.concatenate(
                [jnp.where(lane_head == h, query, zero) for h in range(GROUP)], axis=0
            )
            for k in range(SLOTS // near):
                score_ref[:, k * TILE_KEYS : (k + 1) * TILE_KEYS] = lax.dot_general(
                    stacked, keys_at(p, 0, k), (((1,), (1,)), ((), ())),
                    preferred_element_type=jnp.float32,
                )

        def soften(p, score_ref, weight_ref, total_ref):
            at = p * ENTRY + QUERY_COLS + SLOTS
            kinds = [table_ref[at + pair] for pair in range(PAIRS)]
            lanes = 8 * rows
            for h in range(GROUP):
                for t in range(QUERY_COLS):
                    here = slice((h * QUERY_COLS + t) * rows, (h * QUERY_COLS + t + 1) * rows)
                    parts = [
                        score_ref[here, pair * lanes : (pair + 1) * lanes]
                        + tile_ref[kinds[pair], h * BIAS_STEPS + 2 * pair - t + QUERY_COLS - 1]
                        for pair in range(PAIRS)
                    ]
                    peak = jnp.max(functools.reduce(jnp.maximum, parts), axis=1, keepdims=True)
                    parts = [jnp.exp(part - peak) for part in parts]
                    total = jnp.sum(functools.reduce(jnp.add, parts), axis=1, keepdims=True)
                    for pair in range(PAIRS):
                        weight_ref[here, pair * lanes : (pair + 1) * lanes] = parts[pair].astype(
                            jnp.bfloat16
                        )
                    total_ref[here] = jnp.broadcast_to(total, (rows, GROUP_FEATURES // 2))

        def finish(p, weight_ref, total_ref):
            values = jnp.concatenate(
                [keys_at(p, 1, k) for k in range(SLOTS // near)], axis=0
            )
            summed = jnp.dot(weight_ref[...], values, preferred_element_type=jnp.float32)
            result = summed[:tall]
            total = total_ref[...]
            total = jnp.concatenate([total, total], axis=1)
            share = total[:tall]
            for h in range(1, GROUP):
                part = slice(h * tall, (h + 1) * tall)
                result = jnp.where(lane_head == h, summed[part], result)
                share = jnp.where(lane_head == h, total[part], share)
            row_at = p * tall if isinstance(p, int) else pl.multiple_of(p * tall, tall)
            done_ref[pl.ds(row_at, tall)] = (result / share).astype(
                jnp.bfloat16
            )

        def two(n, carry):
            for side in range(2):
                i = 2 * n + side
                finish(i, weight_refs[side], total_refs[side])
                soften(
                    i + 1, score_refs[1 - side], weight_refs[1 - side], total_refs[1 - side]
                )
                multiply(i + 2, score_refs[side])
            return carry

        steps = blocks + 1
        lax.fori_loop(0, -(-steps // 2), two, 0)
        if steps % 2 == 0:
            finish(LEAD + blocks - 1, weight_refs[(blocks - 1) % 2], total_refs[(blocks - 1) % 2])

        own_ref[g] = jnp.dot(
            place_ref[...], done_ref[LEAD * tall :], preferred_element_type=jnp.float32
        ).astype(jnp.bfloat16)

    start(0, first)
    swap_copy(SWAP).start()
    if groups > 1:
        start(1, first)
    span = cols + 2 * HALO
    wide = spread_ref.shape[1] // 2
    kept = side // spill
    target, packed = iota(spread_ref.shape, 0), iota(spread_ref.shape, 1)
    at, line = target // rows, target % rows
    second_half = packed >= wide
    spot = packed - jnp.where(second_half, wide, 0)
    column = spot // spill
    column = jnp.where(
        spot < edge,
        column + HALO,
        jnp.where(spot < edge + side, column - cols + HALO - kept, column - kept + HALO),
    )
    wanted = jnp.where(second_half, spill, 0) + spot % spill
    spread_ref[...] = ((at == column) & (line == wanted)).astype(jnp.float32).astype(jnp.bfloat16)
    place_ref[...] = (
        iota(place_ref.shape, 1) == jnp.broadcast_to(column_slots((tokens, 1)), place_ref.shape)
    ).astype(jnp.float32).astype(jnp.bfloat16)
    for g in range(2, groups):
        turn(g)
    build_bias(0)
    arrive(0, first)
    start(0, second)
    if groups > 2:
        start(2, first)

    model_tiles = half // GROUP_FEATURES

    def project(g):
        weights = slice(g * GROUP_FEATURES, (g + 1) * GROUP_FEATURES)

        def one(n, carry):
            lanes = pl.ds(pl.multiple_of(n * GROUP_FEATURES, GROUP_FEATURES), GROUP_FEATURES)
            part = jnp.dot(own_ref[g], mine_ref[weights, lanes], preferred_element_type=jnp.float32)
            sum_ref[:, lanes] = part if g == 0 else sum_ref[:, lanes] + part
            return carry

        lax.fori_loop(0, model_tiles, one, 0)

    pass_on, pass_last = min(2, groups - 1), min(5, groups - 1)
    for g in range(groups):
        if g > 0:
            head_copy(g - 1).start()
            build_bias(g)
        if g + 1 < groups:
            arrive(g + 1, first)
            start(g + 1, second)
            if g + 3 < groups:
                start(g + 3, first)
        if g == pass_on:
            swap_copy(SWAP).wait_recv()
            swap_copy(SWAP_ACROSS).start()
            swap_copy(SWAP_MATE).start()
        if g == pass_last:
            swap_copy(SWAP_ACROSS).wait_recv()
            swap_copy(SWAP_LAST).start()
        arrive(g, second)
        unpack_edges(g)
        attend(g)
        if g == 0:
            own_weight.wait()
        project(g)
    head_copy(groups - 1).start()
    swap_copy(SWAP_MATE).wait_recv()
    swap_copy(SWAP_LAST).wait_recv()

    def combine(before, done):
        def one(n, carry):
            lanes = pl.ds(pl.multiple_of(n * GROUP_FEATURES, GROUP_FEATURES), GROUP_FEATURES)
            total = sum_ref[:, lanes]
            for g in before:
                weights = slice(g * GROUP_FEATURES, (g + 1) * GROUP_FEATURES)
                total = total + jnp.dot(
                    other_ref[g], theirs_ref[weights, lanes], preferred_element_type=jnp.float32
                )
            if done:
                out_ref[:, lanes] = total.astype(jnp.bfloat16)
            else:
                sum_ref[:, lanes] = total
            return carry

        lax.fori_loop(0, model_tiles, one, 0)

    for g in range(groups - 1):
        head_copy(g).wait_recv()
    combine(range(groups - 1), False)
    head_copy(groups - 1).wait_recv()
    combine([groups - 1], True)
    for g in range(groups):
        for which in range(COPIES):
            @pl.when(sends[which])
            def _():
                copy(g, which).wait_send()
        head_copy(g).wait_send()
    for which in range(SWAPS):
        swap_copy(which).wait_send()


def fused_layer(dilation, table, bias, query, key, value, weight):
    rows, cols, features = query.shape
    groups = features // GROUP_FEATURES
    tokens = rows * cols
    half = weight.shape[1] // 2
    span = cols + 2 * HALO
    spill = HALO - rows
    edge = spill * cols
    wide = edge + 2 * (-(-spill * HALO // 16) * 16)
    smem = pl.BlockSpec(memory_space=pltpu.SMEM)
    vmem = pl.BlockSpec(memory_space=pltpu.VMEM)
    hbm = pl.BlockSpec(memory_space=pl.ANY)
    blocks = block_count(cols)
    stacked = GROUP * QUERY_COLS * rows
    keys = SLOTS * 4 * rows
    half_type = jnp.bfloat16
    return pl.pallas_call(
        functools.partial(fused_kernel, groups, rows, cols),
        in_specs=[smem, smem, smem, vmem, vmem, vmem, hbm],
        out_specs=vmem,
        out_shape=jax.ShapeDtypeStruct((tokens, half), half_type),
        scratch_shapes=[
            *[pltpu.VMEM((2, span, 4 * rows, GROUP_FEATURES), half_type)] * groups,
            *[pltpu.VMEM((2, 2, wide, GROUP_FEATURES), half_type)] * groups,
            pltpu.VMEM((groups, 2, 2, edge, GROUP_FEATURES), half_type),
            pltpu.VMEM((4, GROUP * BIAS_STEPS, rows, 8 * rows), jnp.float32),
            pltpu.VMEM((stacked, keys), jnp.float32),
            pltpu.VMEM((stacked, keys), jnp.float32),
            pltpu.VMEM((stacked, keys), half_type),
            pltpu.VMEM((stacked, keys), half_type),
            pltpu.VMEM((stacked, GROUP_FEATURES // 2), jnp.float32),
            pltpu.VMEM((stacked, GROUP_FEATURES // 2), jnp.float32),
            pltpu.VMEM((cols, rows, GROUP_FEATURES), half_type),
            pltpu.VMEM(((LEAD + blocks) * QUERY_COLS * rows, GROUP_FEATURES), half_type),
            pltpu.VMEM((tokens + 2 * edge, tokens), half_type),
            pltpu.VMEM((tokens, blocks * QUERY_COLS * rows), half_type),
            pltpu.VMEM((span * rows, 2 * wide), half_type),
            pltpu.VMEM((groups, tokens, GROUP_FEATURES), half_type),
            pltpu.VMEM((groups, tokens, GROUP_FEATURES), half_type),
            pltpu.VMEM((features, half), half_type),
            pltpu.VMEM((features, half), half_type),
            pltpu.VMEM((tokens, half), jnp.float32),
            pltpu.SemaphoreType.DMA((groups, COPIES)),
            pltpu.SemaphoreType.DMA((groups, COPIES)),
            pltpu.SemaphoreType.DMA((SWAPS,)),
            pltpu.SemaphoreType.DMA((SWAPS,)),
            pltpu.SemaphoreType.DMA((groups,)),
            pltpu.SemaphoreType.DMA((groups,)),
            pltpu.SemaphoreType.DMA,
        ],
        compiler_params=pltpu.CompilerParams(
            collective_id=0, has_side_effects=True, vmem_limit_bytes=67043328
        ),
        cost_estimate=pl.CostEstimate(
            flops=groups * blocks * 4 * stacked * keys * GROUP_FEATURES,
            bytes_accessed=query.size * 8,
            transcendentals=groups * blocks * stacked * keys,
        ),
    )(dilation, table, bias, query, key, value, weight)


def block_tables(dilation, rows, cols):
    total_cols = cols * lax.axis_size("col")
    anchor = lax.axis_index("col") * cols
    span = cols + 2 * HALO
    per_class = -(-(-(-cols // dilation)) // QUERY_COLS)
    block = jnp.arange(block_count(cols), dtype=jnp.int32)
    base = block // per_class + (block % per_class) * QUERY_COLS * dilation
    base = base[:, None]
    query_cols = jnp.clip(
        base + jnp.arange(QUERY_COLS, dtype=jnp.int32)[None] * dilation, 0, cols - 1
    )
    key_cols = base + (jnp.arange(SLOTS, dtype=jnp.int32)[None] - RADIUS_MAX) * dilation
    real = (key_cols + anchor >= 0) & (key_cols + anchor < total_cols)
    low, high = real[:, 0::2], real[:, 1::2]
    kind = jnp.where(low, jnp.where(high, 0, 1), jnp.where(high, 2, 3))
    key_cols = jnp.clip(key_cols + HALO, 0, span - 1)
    table = jnp.concatenate([query_cols, key_cols, kind], axis=1).astype(jnp.int32)
    table = jnp.pad(table, ((LEAD, TRAIL), (0, 0)))
    return table.reshape(-1)


def bias_tables(rel_bias, pattern, radius):
    steps = jnp.arange(WINDOW, dtype=jnp.int32) - RADIUS_MAX
    chosen = (pattern == 1) | ((steps[:, None] == 0) & (steps[None, :] == 0))
    chosen = chosen & (jnp.abs(steps)[:, None] <= radius) & (jnp.abs(steps)[None, :] <= radius)
    bias = jnp.where(chosen[None], rel_bias, MASKED)
    before = QUERY_COLS - 1
    bias = jnp.pad(
        bias, ((0, 0), (0, 0), (before, TABLE_STEPS - WINDOW - before)), constant_values=MASKED
    )
    return bias.reshape(-1)


def shards(
    query_map, key_map, value_map, window_mask, tile_radius, dilation_per_tile, rel_bias, out_weight
):
    rows, cols, features = query_map.shape
    dilation = dilation_per_tile[0, 0]
    table = block_tables(dilation, rows, cols)
    bias = bias_tables(rel_bias, window_mask[0, 0], tile_radius[0, 0])
    mixed = fused_layer(
        dilation.reshape(1), table, bias, query_map, key_map, value_map, out_weight
    )
    return mixed.reshape(rows, cols, out_weight.shape[1] // 2)


def solution(mesh):
    placed = (
        P("row", "col", "head"),
        P("row", "col", "head"),
        P("row", "col", "head"),
        P("row", "col", None, None),
        P("row", "col"),
        P("row", "col"),
        P("head", None, None),
        P("head", None),
    )
    return jax.shard_map(
        shards, mesh=mesh, in_specs=placed, out_specs=P("row", "col", "head"), check_vma=False
    )
```
